32 devices in a mesh: fsdp: 8 (over y, x, core), dp: 4 (over z).
Axes of the slice: x: 2, y: 2, z: 4, core: 2. Of those that a mesh axis runs over, the one named last changes fastest.
Arguments:
- tokens: bfloat16 [16384, 4096], P(('fsdp', 'dp')), may hold values from -40 to 40
- cotangent: bfloat16 [16384, 2048], P(('fsdp', 'dp')), may hold values from -20 to 20
- weight: bfloat16 [4096, 2048], P('fsdp'), may hold values from -1 to 1
- left_vector: float32 [4096], P('fsdp'), may hold values from -6 to 6
Outputs:
- layer_out: bfloat16 [16384, 2048], P(('fsdp', 'dp'))
- input_grad: bfloat16 [16384, 4096], P(('fsdp', 'dp'))
- update: bfloat16 [4096, 2048], P('fsdp')
- left_next: float32 [4096], P('fsdp')
- right_next: float32 [2048], replicated
The draws below stay inside these ranges and needn't reach their ends.
All inputs are finite; a program needn't handle non-finite values.
Results may differ from the reference program's by a relative error of at most 0.015.
Values may be sent and summed in bfloat16 or wider, within the bound.
A program may use at most 128 MiB of HBM per device.

```python
import math
import jax
import jax.numpy as jnp
from jax import lax

D = 4096
TOK_DEV = 512
OUT = 2048
TOKENS = 16384
N_FSDP = 8


token_share = 3.0


cotangent_share = 3.0


spike_gain = 3.0


def base_values(key, rows, columns):
    values = jnp.clip(jax.random.normal(key, (rows, columns), jnp.float32), -6.0, 6.0)
    return values


def common_parts(key):
    weight_key = jax.random.fold_in(key, 11)
    direction_key = jax.random.fold_in(key, 12)
    latent_key = jax.random.fold_in(key, 13)
    weight_raw = base_values(weight_key, D, OUT)
    weight_value = (weight_raw * (1.0 / math.sqrt(D))).astype(jnp.bfloat16).astype(jnp.float32)
    direction = jax.random.normal(direction_key, (D,), jnp.float32)
    direction = direction / jnp.sqrt(jnp.sum(direction * direction))
    latent = jnp.clip(jax.random.normal(latent_key, (TOKENS,), jnp.float32), -4.0, 4.0)
    return (weight_value, direction, latent)


def draw_weight(key, part):
    weight_value, direction, latent = common_parts(key)
    return weight_value.astype(jnp.bfloat16)


def draw_tokens(key, part):
    weight_value, direction, latent = common_parts(key)
    random_key = jax.random.fold_in(key, 21)
    pairing_key = jax.random.fold_in(key, 22)
    values = base_values(random_key, TOKENS, D)
    block_count = TOKENS // TOK_DEV
    pairing = (jax.random.permutation(pairing_key, block_count) % N_FSDP).astype(jnp.int32)
    row_block = (jnp.arange(TOKENS) // TOK_DEV).astype(jnp.int32)
    column_block = (jnp.arange(D) // (D // N_FSDP)).astype(jnp.int32)
    paired = pairing[row_block]
    boost = 1.0 + spike_gain * (paired[:, None] == column_block[None, :]).astype(jnp.float32)
    values = values * boost + token_share * latent[:, None] * direction[None, :]
    return values.astype(jnp.bfloat16)


def draw_cotangent(key, part):
    weight_value, direction, latent = common_parts(key)
    random_key = jax.random.fold_in(key, 31)
    along = jnp.dot(direction, weight_value, precision=lax.Precision.HIGHEST)
    along = along / jnp.sqrt(jnp.sum(along * along))
    values = base_values(random_key, TOKENS, OUT)
    values = values + cotangent_share * latent[:, None] * along[None, :]
    return values.astype(jnp.bfloat16)


def shard_levels(rng, shape, cuts, low, high):
    factor_of, own = 1.0, jax.random.fold_in(rng, 6)
    for axis_at, shards_of in cuts:
        heights = jnp.exp(jax.random.uniform(jax.random.fold_in(own, axis_at), (shards_of,), jnp.float32, low / len(cuts), high / len(cuts)))
        factor_of = factor_of * jnp.repeat(heights, shape[axis_at] // shards_of).reshape([-1 if axis == axis_at else 1 for axis in range(len(shape))])
    return factor_of


def centred(own_key, extent, width, bound, shards=(), held_as=jnp.bfloat16):
    entries = jax.random.normal(own_key, extent, jnp.float32) * width
    if len(shards) > 0:
        entries = shard_levels(own_key, extent, shards, -0.22, 0.18) * entries
    return jnp.clip(entries, min=-bound, max=bound).astype(held_as)


def setup_inputs(seed: int = 0) -> dict:
    key_of = jax.random.split(jax.random.key(seed), 5)
    return {
        "tokens": draw_tokens(jax.random.fold_in(key_of[4], 71), 0),
        "cotangent": draw_cotangent(jax.random.fold_in(key_of[4], 71), 0),
        "weight": draw_weight(jax.random.fold_in(key_of[4], 71), 0),
        "left_vector": centred(key_of[3], (D,), 1.0, 6.0, ((0, 8),), jnp.float32),
    }


epsilon = 1e-06

def reference(tokens, cotangent, weight, left_vector):
    highest = lax.Precision.HIGHEST
    weight_wide = weight.astype(jnp.float32)
    right_raw = jnp.dot(left_vector, weight_wide, precision=highest)
    right_next = right_raw / jnp.sqrt(jnp.sum(right_raw * right_raw) + epsilon)
    left_raw = jnp.dot(weight_wide, right_next, precision=highest)
    left_sq = jnp.sum(left_raw * left_raw)
    spectral = jnp.sqrt(left_sq + epsilon)
    left_next = left_raw / spectral
    block_count = TOKENS // TOK_DEV
    tok_blocks = tokens.reshape(block_count, TOK_DEV, D)
    cot_blocks = cotangent.reshape(block_count, TOK_DEV, OUT)

    def accumulate(running, pieces):
        tok_block, cot_block = pieces
        out_block = (jnp.dot(tok_block, weight, preferred_element_type=jnp.float32) / spectral).astype(jnp.bfloat16)
        back_prod = lax.dot_general(cot_block, weight, (((1,), (1,)), ((), ())), preferred_element_type=jnp.float32)
        back_block = (back_prod / spectral).astype(jnp.bfloat16)
        term_block = lax.dot_general(tok_block, cot_block, (((0,), (0,)), ((), ())), preferred_element_type=jnp.float32)
        term_block = lax.optimization_barrier(term_block.astype(jnp.bfloat16)).astype(jnp.float32)
        return (running + term_block, (out_block, back_block))
    grad_sum, (out_all, back_all) = lax.scan(accumulate, jnp.zeros((D, OUT), jnp.float32), (tok_blocks, cot_blocks))
    inner_prod = jnp.sum(grad_sum * weight_wide)
    rank_coeff = inner_prod / (spectral * spectral)
    gradient = grad_sum / spectral - rank_coeff * left_next[:, None] * right_next[None, :]
    grad_rms = jnp.sqrt(jnp.mean(gradient * gradient) + epsilon)
    update = (gradient / grad_rms).astype(jnp.bfloat16)
    layer_out = out_all.reshape(TOKENS, OUT)
    input_grad = back_all.reshape(TOKENS, D)
    return (layer_out, input_grad, update, left_next, right_next)
```

```python
import functools

import jax
import jax.numpy as jnp
from jax import lax
from jax.experimental import pallas as pl
from jax.experimental.pallas import tpu as pltpu
from jax.sharding import PartitionSpec as P

epsilon = 1e-06


def swap(value, bit):
    size = lax.axis_size("fsdp")
    return lax.ppermute(value, "fsdp", [(i, i ^ (1 << bit)) for i in range(size)])


def total_kernel(part_ref, sum_ref, slots, send_sem, recv_sem):
    size = slots.shape[0]
    me = lax.axis_index("fsdp")
    barrier = pltpu.get_barrier_semaphore()
    for step in range(1, size):
        pl.semaphore_signal(
            barrier,
            inc=1,
            device_id={"fsdp": lax.rem(me + step, size)},
            device_id_type=pl.DeviceIdType.MESH,
        )
    pl.semaphore_wait(barrier, size - 1)

    def copy(step):
        return pltpu.make_async_remote_copy(
            src_ref=part_ref,
            dst_ref=slots.at[me],
            send_sem=send_sem.at[step],
            recv_sem=recv_sem.at[step],
            device_id={"fsdp": lax.rem(me + step, size)},
            device_id_type=pl.DeviceIdType.MESH,
        )

    for step in range(1, size):
        copy(step).start()
    slots[me] = part_ref[...]
    for step in range(1, size):
        copy(step).wait()
    sum_ref[...] = jnp.sum(slots[...], axis=0)


def total(part, collective_id):
    size = lax.axis_size("fsdp")
    return pl.pallas_call(
        total_kernel,
        out_shape=jax.ShapeDtypeStruct(part.shape, part.dtype),
        in_specs=[pl.BlockSpec(memory_space=pltpu.VMEM)],
        out_specs=pl.BlockSpec(memory_space=pltpu.VMEM),
        scratch_shapes=[
            pltpu.VMEM((size, *part.shape), part.dtype),
            pltpu.SemaphoreType.DMA((size,)),
            pltpu.SemaphoreType.DMA((size,)),
        ],
        compiler_params=pltpu.CompilerParams(collective_id=collective_id, has_side_effects=True),
        cost_estimate=pl.CostEstimate(flops=0, bytes_accessed=2**22, transcendentals=0),
    )(part)


def lanes(*scalars):
    rows = jnp.arange(8)[:, None]
    return sum(jnp.where(rows == i, s, 0.0) for i, s in enumerate(scalars)) + jnp.zeros((8, 128))


def replica_sum(part, group):
    size = lax.axis_size("dp")
    me = lax.axis_index("dp")
    order = list(range(size.bit_length() - 1))
    if group % 2 == 1:
        order.reverse()

    def across(value, bit):
        return lax.ppermute(value, "dp", [(i, i ^ (1 << bit)) for i in range(size)])

    for bit in order:
        mine = jnp.bitwise_and(jnp.right_shift(me, bit), 1)
        rows = part.shape[0] // 2
        kept = lax.dynamic_slice_in_dim(part, mine * rows, rows, axis=0)
        sent = lax.dynamic_slice_in_dim(part, (1 - mine) * rows, rows, axis=0)
        part = kept + across(sent.astype(jnp.bfloat16), bit).astype(jnp.float32)
    part = part.astype(jnp.bfloat16)
    for bit in reversed(order):
        mine = jnp.bitwise_and(jnp.right_shift(me, bit), 1)
        other = across(part, bit)
        low = jnp.where(mine == 0, part, other)
        high = jnp.where(mine == 0, other, part)
        part = jnp.concatenate([low, high], axis=0)
    return part


def project_kernel(base, count, first, last, *refs):
    scale_ref, tokens, cotangent = refs[:3]
    pieces = refs[3 : 3 + 2 * count]
    rest = list(refs[3 + 2 * count :])
    if not first:
        acc_in, _ = rest[:2]
        rest = rest[2:]
    out_ref, back_ref = rest[:2]
    tok_v, cot_v, w_v, back_v, acc, tok_sem, w_sem, back_sem, cot_sem = rest[2:11]
    me = lax.axis_index("fsdp")
    half, _ = pieces[0].shape
    rows = 2 * half

    def columns(k):
        start = jnp.bitwise_xor(me, base + k) * rows
        return pl.ds(pl.multiple_of(start, rows), rows)

    def load_tok(k):
        return pltpu.make_async_copy(tokens.at[:, columns(k)], tok_v.at[k], tok_sem.at[k])

    def load_w(piece, k, side):
        return pltpu.make_async_copy(
            piece, w_v.at[k, pl.ds(side * half, half)], w_sem.at[k, side]
        )

    def store_back(k):
        return pltpu.make_async_copy(back_v.at[k], back_ref.at[:, columns(k)], back_sem.at[k])

    load_cot = pltpu.make_async_copy(cotangent, cot_v, cot_sem.at[0])
    for k in range(count):
        load_tok(k).start()
        for side in (0, 1):
            load_w(pieces[2 * k + side], k, side).start()
        if k == 0:
            load_cot.start()
    if first:
        acc[...] = jnp.zeros_like(acc)
    else:
        load_acc = pltpu.make_async_copy(acc_in, acc, cot_sem.at[1])
        load_acc.start()
        load_acc.wait()
    load_cot.wait()
    scale = scale_ref[0]

    @pl.loop(0, count)
    def _(k):
        load_tok(k).wait()
        load_w(pieces[0], k, 0).wait()
        load_w(pieces[1], k, 1).wait()
        acc[...] += jnp.dot(tok_v[k], w_v[k], preferred_element_type=jnp.float32)
        back = lax.dot_general(
            cot_v[...], w_v[k], (((1,), (1,)), ((), ())), preferred_element_type=jnp.float32
        )
        back_v[k] = (back * scale).astype(back_v.dtype)
        store_back(k).start()

    if last:
        out_ref[...] = (acc[...] * scale).astype(out_ref.dtype)
    else:
        out_ref[...] = acc[...]

    @pl.loop(0, count)
    def _(k):
        store_back(k).wait()


def project(scale, tokens, cotangent, pieces, base, carry, last):
    count = len(pieces) // 2
    toks, width = tokens.shape
    outs = cotangent.shape[1]
    rows = 2 * pieces[0].shape[0]
    any_space = pl.BlockSpec(memory_space=pl.ANY)
    first = carry is None
    operands = [scale, tokens, cotangent, *pieces] + ([] if first else list(carry))
    in_specs = [pl.BlockSpec(memory_space=pltpu.SMEM)] + [any_space] * (len(operands) - 1)
    return pl.pallas_call(
        functools.partial(project_kernel, base, count, first, last),
        out_shape=(
            jax.ShapeDtypeStruct((toks, outs), jnp.bfloat16 if last else jnp.float32),
            jax.ShapeDtypeStruct((toks, width), jnp.bfloat16),
        ),
        in_specs=in_specs,
        out_specs=(pl.BlockSpec(memory_space=pltpu.VMEM), any_space),
        scratch_shapes=[
            pltpu.VMEM((count, toks, rows), jnp.bfloat16),
            pltpu.VMEM((toks, outs), jnp.bfloat16),
            pltpu.VMEM((count, rows, outs), jnp.bfloat16),
            pltpu.VMEM((count, toks, rows), jnp.bfloat16),
            pltpu.VMEM((toks, outs), jnp.float32),
            pltpu.SemaphoreType.DMA((count,)),
            pltpu.SemaphoreType.DMA((count, 2)),
            pltpu.SemaphoreType.DMA((count,)),
            pltpu.SemaphoreType.DMA((2,)),
        ],
        input_output_aliases={} if first else {len(operands) - 1: 1},
        compiler_params=pltpu.CompilerParams(vmem_limit_bytes=56 * 2**20),
        cost_estimate=pl.CostEstimate(
            flops=4 * count * rows * toks * outs,
            bytes_accessed=2 * count * rows * (outs + 2 * toks) + 4 * toks * outs,
            transcendentals=0,
        ),
    )(*operands)


def step(tokens, cotangent, weight, left_vector):
    highest = lax.Precision.HIGHEST
    wide, narrow = jnp.float32, jnp.bfloat16
    size = lax.axis_size("fsdp")
    bits = size.bit_length() - 1
    me = lax.axis_index("fsdp")
    shard_rows, outs = weight.shape
    half = shard_rows // 2
    orders = (tuple(range(1, bits)), tuple(range(bits - 1, 0, -1)))

    def token_block(rel):
        start = jnp.bitwise_xor(me, rel) * shard_rows
        return lax.dynamic_slice_in_dim(tokens, start, shard_rows, axis=1)

    evens = [rel for rel in range(size) if rel % 2 == 0]
    cot_chip = jnp.concatenate([cotangent, swap(cotangent, 0)], axis=0)
    tok_chip = {
        rel: jnp.concatenate([token_block(rel), swap(token_block(rel | 1), 0)], axis=0)
        for rel in reversed(evens)
    }

    weight_wide = weight.astype(wide)
    part_right = jnp.dot(left_vector, weight_wide, precision=highest)
    right_raw = total(part_right.reshape(outs // 128, 128), 1).reshape(outs)
    right_next = right_raw / jnp.sqrt(jnp.sum(right_raw * right_raw) + epsilon)
    left_raw = jnp.dot(weight_wide, right_next, precision=highest)
    left_sq = total(lanes(jnp.sum(left_raw * left_raw)), 2)[0, 0]
    spectral = jnp.sqrt(left_sq + epsilon)
    left_next = left_raw / spectral

    sides = (0, 1)
    cot_chip, tok_chip, left_sq = lax.optimization_barrier((cot_chip, tok_chip, left_sq))

    groups = 2
    group_cols = outs // groups
    live = {}
    for group in range(groups):
        cot_part = cot_chip[:, group * group_cols : (group + 1) * group_cols]
        for side in sides:
            live[group, side] = {
                rel: lax.dot_general(
                    tok_chip[rel][:, side * half : (side + 1) * half],
                    cot_part,
                    (((0,), (0,)), ((), ())),
                    preferred_element_type=wide,
                ).astype(narrow)
                for rel in reversed(evens)
            }
    for phase in range(bits - 1):
        for group in range(groups):
            for side in sides:
                mask = 1 << orders[side][phase]
                now = live[group, side]
                live[group, side] = {
                    rel: now[rel].astype(wide)
                    + swap(now[rel | mask].astype(narrow), orders[side][phase]).astype(wide)
                    for rel in sorted(now)
                    if not rel & mask
                }
    grad_parts = [
        replica_sum(
            jnp.concatenate([live[group, side][0] for side in sides], axis=0), group
        )
        for group in range(groups)
    ]
    grad_sum = jnp.concatenate(grad_parts, axis=1).astype(wide)

    own_a, own_b, _ = lax.optimization_barrier(
        (weight[:half], weight[half:], [live[0, side][0] for side in sides])
    )
    held = ({0: own_a}, {0: own_b})
    for side in sides:
        for bit in orders[side]:
            for rel in sorted(held[side]):
                held[side][rel | (1 << bit)] = swap(held[side][rel], bit)
    for side in sides:
        for rel in sorted(held[side]):
            held[side][rel | 1] = swap(held[side][rel], 0)

    entry_count = shard_rows * size * outs
    outer = left_next[:, None] * right_next[None, :]
    sums = total(
        lanes(
            jnp.sum(grad_sum * grad_sum),
            jnp.sum(grad_sum * weight_wide),
            jnp.sum(grad_sum * outer),
        ),
        3,
    )
    grad_sq_raw, inner_prod, cross_term = sums[0, 0], sums[1, 0], sums[2, 0]
    rank_coeff = inner_prod / (spectral * spectral)
    gradient = grad_sum / spectral - rank_coeff * outer
    left_unit = left_sq / (left_sq + epsilon)
    right_unit = jnp.sum(right_next * right_next)
    grad_sq = (
        grad_sq_raw / (spectral * spectral)
        - 2.0 * rank_coeff * cross_term / spectral
        + rank_coeff * rank_coeff * left_unit * right_unit
    )
    grad_rms = jnp.sqrt(grad_sq / entry_count + epsilon)
    update = (gradient / grad_rms).astype(narrow)

    scale = (1.0 / spectral).reshape(1)
    near, far = range(size - 2), range(size - 2, size)
    halves = lambda rels: [held[side][rel] for rel in rels for side in (0, 1)]
    carry = project(scale, tokens, cotangent, halves(near), 0, None, False)
    layer_out, input_grad = project(scale, tokens, cotangent, halves(far), size - 2, carry, True)
    return (layer_out, input_grad, update, left_next, right_next)


def solution(mesh):
    placed = (P(("fsdp", "dp"), None), P(("fsdp", "dp"), None), P("fsdp", None), P("fsdp"))
    return jax.shard_map(
        step,
        mesh=mesh,
        in_specs=placed,
        out_specs=(
            P(("fsdp", "dp"), None),
            P(("fsdp", "dp"), None),
            P("fsdp", None),
            P("fsdp"),
            P(),
        ),
        check_vma=False,
    )
```
